32 devices in a mesh: seq: 8 (over z, y), grp: 4 (over x, core).
Axes of the slice: x: 2, y: 2, z: 4, core: 2. Of those that a mesh axis runs over, the one named last changes fastest.
Arguments:
- tokens: bfloat16 [4096, 2560], P('seq'), may hold values from -6 to 6
- norm_gain: float32 [2560], replicated, may hold values from 0.25 to 1.75
- inner_weight: bfloat16 [2560, 2, 5120], P(None, None, ('grp', 'seq')), may hold values from -0.125 to 0.125
- state_weight: bfloat16 [2560, 2, 128], replicated, may hold values from -0.125 to 0.125
- step_weight: bfloat16 [2560, 80], P(None, 'grp'), may hold values from -0.125 to 0.125
- step_bias: float32 [80], P('grp'), may hold values from -1 to 1
- decay_rate: float32 [80], P('grp'), may hold values from 4.8828124e-06 to 0.05
- skip_scale: float32 [80], P('grp'), may hold values from 0.5 to 1.5
- conv_inner: bfloat16 [4, 5120], P(None, 'grp'), may hold values from -3 to 3
- conv_state: bfloat16 [4, 2, 128], replicated, may hold values from -3 to 3
- out_gain: float32 [5120], P('grp'), may hold values from 0.25 to 1.75
- out_weight: bfloat16 [5120, 2560], P(None, 'grp'), may hold values from -0.078125 to 0.078125
Outputs:
- mixed: bfloat16 [4096, 2560], P('seq', 'grp')
The draws below stay inside these ranges and needn't reach their ends.
All inputs are finite; a program needn't handle non-finite values.
Results may differ from the reference program's by a relative error of at most 0.0075.
Values may be sent and summed in bfloat16 or wider, within the bound.
A program may use at most 64 MiB of HBM per device.

```python
import math
from functools import partial
import jax
import jax.numpy as jnp
from jax import lax

D = 2560
D_INNER = 5120
HEADS = 80
HEAD_DIM = 64
D_STATE = 128
SPAN = 256
KERNEL = 4
SEQ_LEN = 4096


def block_levels(key, dims, cuts, smallest, high):
    def one(position, parts):
        draws = jax.random.uniform(jax.random.fold_in(jax.random.fold_in(key, 6), position), (parts,), jnp.float32, smallest / len(cuts), high / len(cuts))
        return jnp.repeat(jnp.exp(draws), dims[position] // parts).reshape((-1,) + (1,) * (len(dims) - position - 1))

    gain = one(*cuts[0])
    for cut in cuts[1:]:
        gain = gain * one(*cut)
    return gain


def bell_draw(rng, extent, scale, limit, split=(), held_as=jnp.bfloat16):
    level = block_levels(rng, extent, split, -0.22, 0.18) if split else 1.0
    drawn = jax.random.normal(rng, extent, jnp.float32) * scale * level
    return jnp.minimum(jnp.maximum(drawn, -limit), limit).astype(held_as)


def setup_inputs(seed: int = 0) -> dict:
    seeds = jax.random.split(jax.random.key(seed), 13)
    return {
        "tokens": bell_draw(seeds[0], (SEQ_LEN, D), 1.0, 6.0, ((0, 8),)),
        "norm_gain": jnp.clip(1.0 + 0.15 * jax.random.normal(seeds[1], (D,), jnp.float32), 0.25, 1.75),
        "inner_weight": bell_draw(seeds[2], (D, 2, D_INNER), D ** -0.5, 0.125, ((2, 32),)),
        "state_weight": bell_draw(seeds[3], (D, 2, D_STATE), D ** -0.5, 0.125),
        "step_weight": bell_draw(seeds[4], (D, HEADS), D ** -0.5, 0.125, ((1, 4),)),
        "step_bias": jnp.clip(jax.random.uniform(seeds[5], (HEADS,), jnp.float32, -1.0, 1.0) * block_levels(seeds[5], (HEADS,), ((0, 4),), -0.4, 0.0), -1.0, 1.0),
        "decay_rate": jnp.clip(jnp.exp(math.log(0.05) - 9.2340569 * jax.random.uniform(seeds[6], (HEADS,), jnp.float32) ** block_levels(seeds[6], (HEADS,), ((0, 4),), -0.2, 0.2)), 4.882812390860636e-06, 0.05),
        "skip_scale": jnp.clip(0.5 + 1.0 * jax.random.uniform(seeds[7], (HEADS,), jnp.float32) ** block_levels(seeds[7], (HEADS,), ((0, 4),), -0.2, 0.2), 0.5, 1.5),
        "conv_inner": bell_draw(seeds[8], (KERNEL, D_INNER), KERNEL ** -0.5, 3.0, ((1, 4),)),
        "conv_state": bell_draw(seeds[9], (KERNEL, 2, D_STATE), KERNEL ** -0.5, 3.0),
        "out_gain": jnp.clip(1.0 + 0.15 * jax.random.normal(seeds[10], (D_INNER,), jnp.float32), 0.25, 1.75),
        "out_weight": bell_draw(seeds[11], (D_INNER, D), D_INNER ** -0.5, 0.078125, ((1, 4),)),
    }


EPS = 1e-05
HIGH = lax.Precision.HIGHEST

def causal_conv(current, weight):
    width = weight.shape[0]
    before = jnp.zeros((width - 1,) + current.shape[1:], current.dtype)
    padded = jnp.concatenate([before, current], axis=0).astype(jnp.float32)
    length = current.shape[0]
    total = jnp.zeros(current.shape, jnp.float32)
    for offset in range(width):
        total = total + weight[offset].astype(jnp.float32) * padded[offset:offset + length]
    return jax.nn.silu(total).astype(jnp.bfloat16)

def span_step(rate, skip, state, inputs):
    xvals, bmat, cmat, delta = inputs
    logdec = -delta * rate[None, :]
    cumul = jnp.cumsum(logdec, axis=0)
    length = cumul.shape[0]
    scores = jnp.einsum('tn,sn->ts', cmat.astype(jnp.float32), bmat.astype(jnp.float32), precision=HIGH)
    lower = jnp.arange(length)[:, None] >= jnp.arange(length)[None, :]
    diffs = cumul.T[:, :, None] - cumul.T[:, None, :]
    decay = jnp.exp(jnp.where(lower[None], diffs, -jnp.inf))
    mixer = (scores[None] * decay * delta.T[:, None, :]).astype(jnp.bfloat16)
    xwide = xvals.astype(jnp.float32)
    intra = jnp.einsum('hts,shp->thp', mixer.astype(jnp.float32), xwide, precision=HIGH)
    inter = jnp.exp(cumul)[:, :, None] * jnp.einsum('tn,hpn->thp', cmat.astype(jnp.float32), state, precision=HIGH)
    output = intra + inter + skip[None, :, None] * xwide
    tail = jnp.exp(cumul[-1][None, :] - cumul) * delta
    weighted = (tail[:, :, None] * bmat.astype(jnp.float32)[:, None, :]).astype(jnp.bfloat16)
    update = jnp.einsum('shp,shn->hpn', xwide, weighted.astype(jnp.float32), precision=HIGH)
    new_state = jnp.exp(cumul[-1])[:, None, None] * state + update
    return (new_state, output)

def reference(tokens, norm_gain, inner_weight, state_weight, step_weight, step_bias, decay_rate, skip_scale, conv_inner, conv_state, out_gain, out_weight):
    length = tokens.shape[0]
    wide = tokens.astype(jnp.float32)
    normed = (wide * lax.rsqrt(lax.optimization_barrier(jnp.mean(wide * wide, axis=1, keepdims=True)) + EPS) * norm_gain).astype(jnp.bfloat16)
    normed_wide = normed.astype(jnp.float32)
    inner = jnp.dot(normed_wide, inner_weight.reshape(D, 2 * D_INNER).astype(jnp.float32), precision=HIGH)
    inner = inner.astype(jnp.bfloat16).reshape(length, 2, D_INNER)
    state_pre = jnp.dot(normed_wide, state_weight.reshape(D, 2 * D_STATE).astype(jnp.float32), precision=HIGH)
    state_pre = state_pre.astype(jnp.bfloat16).reshape(length, 2, D_STATE)
    delta = jax.nn.softplus(jnp.dot(normed_wide, step_weight.astype(jnp.float32), precision=HIGH) + step_bias)
    values = causal_conv(inner[:, 0, :], conv_inner)
    conv_out = causal_conv(state_pre, conv_state)
    blocks = length // SPAN
    xs_blocks = values.reshape(blocks, SPAN, HEADS, HEAD_DIM)
    b_blocks = conv_out[:, 0, :].reshape(blocks, SPAN, D_STATE)
    c_blocks = conv_out[:, 1, :].reshape(blocks, SPAN, D_STATE)
    d_blocks = delta.reshape(blocks, SPAN, HEADS)
    initial = jnp.zeros((HEADS, HEAD_DIM, D_STATE), jnp.float32)
    _, outputs = lax.scan(partial(span_step, decay_rate, skip_scale), initial, (xs_blocks, b_blocks, c_blocks, d_blocks))
    mixed_heads = outputs.reshape(length, D_INNER)
    gated = mixed_heads * jax.nn.silu(inner[:, 1, :].astype(jnp.float32))
    meansq = lax.optimization_barrier(jnp.mean(gated * gated, axis=1))
    scaled = (gated * out_gain).astype(jnp.bfloat16)
    projected = jnp.dot(scaled.astype(jnp.float32), out_weight.astype(jnp.float32), precision=HIGH)
    return (projected * lax.rsqrt(meansq + EPS)[:, None]).astype(jnp.bfloat16)
```

```python
import functools

import jax
import jax.numpy as jnp
from jax import lax
from jax.experimental import pallas as pl
from jax.experimental.pallas import tpu as pltpu
from jax.sharding import PartitionSpec as P

SPAN = 256
HEAD = 64
EPS = 1e-05
CORES = 2
MESH = pl.DeviceIdType.MESH
F32 = jnp.float32
BF16 = jnp.bfloat16


def places(outer, inner, grp):
    s = lax.axis_index("seq")
    g = lax.axis_index("grp")
    return lax.div(s, inner), lax.rem(s, inner), lax.div(g, CORES), lax.rem(g, CORES)


def greet(peers):
    barrier = pltpu.get_barrier_semaphore()
    for peer in peers:
        pl.semaphore_signal(barrier, inc=1, device_id=peer, device_id_type=MESH)
    pl.semaphore_wait(barrier, len(peers))


def remote(src, dst, send, recv, peer):
    return pltpu.make_async_remote_copy(
        src_ref=src, dst_ref=dst, send_sem=send, recv_sem=recv, device_id=peer, device_id_type=MESH
    )


def project_kernel(
    outer, inner, grp, n_ref, w_ref, ws_ref, o_ref, os_ref,
    tok, wbuf, wsend, wrecv, zsend, zrecv, xsend, xrecv, csend, crecv,
):
    z, q, x, c = places(outer, inner, grp)
    chips = grp // CORES
    s, g = z * inner + q, x * CORES + c
    rows = n_ref.shape[0]
    part = rows // grp
    mate = {"grp": x * CORES + 1 - c}

    def at_z(j):
        return {"seq": lax.rem(z + j, outer) * inner + q}

    def at_q(i):
        return {"seq": z * inner + lax.rem(q + i, inner)}

    def at_x(i):
        return {"grp": lax.rem(x + i, chips) * CORES + c}

    peers = (
        [at_z(j) for j in range(1, outer)]
        + [at_q(i) for i in range(1, inner)]
        + [at_x(i) for i in range(1, chips)]
        + [mate]
    )
    greet(peers)

    def piece(index):
        return pl.ds(pl.multiple_of(index * part, part), part)

    zc = {
        j: remote(n_ref.at[piece(g)], tok.at[j - 1, piece(g)], zsend.at[j - 1], zrecv.at[j - 1], at_z(j))
        for j in range(1, outer)
    }
    wc = {
        i: remote(w_ref, wbuf.at[i - 1], wsend.at[i - 1], wrecv.at[i - 1], at_q(i))
        for i in range(1, inner)
    }
    for j in range(1, outer):
        zc[j].start()
    for i in range(1, inner):
        wc[i].start()

    tile = min(256, rows)

    def multiply(j, pick):
        zs = lax.rem(z - j + outer, outer)

        def some(r, carry):
            at = pl.ds(pl.multiple_of(r * tile, tile), tile)
            a = n_ref[at, :] if j == 0 else tok[j - 1, at, :]
            if pick == "state":
                os_ref[zs, at, :] = jnp.dot(a, ws_ref[...], preferred_element_type=F32)
            elif pick == "own":
                o_ref[q, zs, at, :] = jnp.dot(a, w_ref[...], preferred_element_type=F32).astype(BF16)
            else:
                for i in range(1, inner):
                    qs = lax.rem(q - i + inner, inner)
                    o_ref[qs, zs, at, :] = jnp.dot(
                        a, wbuf[i - 1], preferred_element_type=F32
                    ).astype(BF16)
            return carry

        lax.fori_loop(0, rows // tile, some, 0)

    xc, cc = {}, {}

    def on_z(j):
        zc[j].wait_recv()
        here = tok.at[j - 1, piece(g)]
        for i in range(1, chips):
            xc[j, i] = remote(here, here, xsend.at[j - 1, i - 1], xrecv.at[j - 1, i - 1], at_x(i))
            xc[j, i].start()
        cc[j, 0] = remote(here, here, csend.at[j - 1, 0], crecv.at[j - 1, 0], mate)
        cc[j, 0].start()

    def on_x(j):
        for i in range(1, chips):
            xc[j, i].wait_recv()
            there = lax.rem(x - i + chips, chips) * CORES + c
            here = tok.at[j - 1, piece(there)]
            cc[j, i] = remote(here, here, csend.at[j - 1, i], crecv.at[j - 1, i], mate)
            cc[j, i].start()

    multiply(0, "state")
    multiply(0, "own")
    for j in range(1, outer):
        on_z(j)
        if j > 1:
            on_x(j - 1)
    for i in range(1, inner):
        wc[i].wait_recv()
    multiply(0, "other")
    for j in range(1, outer):
        if j == outer - 1:
            on_x(j)
        for i in range(chips):
            cc[j, i].wait_recv()
        multiply(j, "state")
        multiply(j, "own")
        multiply(j, "other")
    for j in range(1, outer):
        zc[j].wait_send()
        for i in range(1, chips):
            xc[j, i].wait_send()
        for i in range(chips):
            cc[j, i].wait_send()
    for i in range(1, inner):
        wc[i].wait_send()


def vmem():
    return pl.BlockSpec(memory_space=pltpu.VMEM)


def project(outer, inner, grp, normed, weight, small):
    rows, depth = normed.shape
    chips = grp // CORES
    dma = pltpu.SemaphoreType.DMA
    hops = max(1, chips - 1)
    return pl.pallas_call(
        functools.partial(project_kernel, outer, inner, grp),
        out_shape=(
            jax.ShapeDtypeStruct((inner, outer, rows, weight.shape[1]), BF16),
            jax.ShapeDtypeStruct((outer, rows, small.shape[1]), F32),
        ),
        in_specs=[vmem()] * 3,
        out_specs=(vmem(), vmem()),
        scratch_shapes=[
            pltpu.VMEM((outer - 1, rows, depth), BF16),
            pltpu.VMEM((inner - 1,) + weight.shape, BF16),
            dma((inner - 1,)),
            dma((inner - 1,)),
            dma((outer - 1,)),
            dma((outer - 1,)),
            dma((outer - 1, hops)),
            dma((outer - 1, hops)),
            dma((outer - 1, chips)),
            dma((outer - 1, chips)),
        ],
        compiler_params=pltpu.CompilerParams(
            collective_id=0, has_side_effects=True, vmem_limit_bytes=60000 * 1024
        ),
        name="project",
    )(normed, weight, small)


def state_kernel(heads, x_ref, b_ref, t_ref, u_ref):
    b = b_ref[...].astype(F32)
    for h in range(heads):
        w = (t_ref[:, h : h + 1] * b).astype(BF16)
        u_ref[h * HEAD : (h + 1) * HEAD, :] = lax.dot_general(
            x_ref[:, h * HEAD : (h + 1) * HEAD], w, (((0,), (0,)), ((), ())), preferred_element_type=F32
        )


def intra_kernel(heads, x_ref, b_ref, c_ref, cc_ref, cr_ref, dr_ref, y_ref):
    span = x_ref.shape[0]
    scores = lax.dot_general(
        c_ref[...], b_ref[...], (((1,), (1,)), ((), ())), preferred_element_type=F32
    )
    lower = lax.broadcasted_iota(jnp.int32, (span, span), 0) >= lax.broadcasted_iota(
        jnp.int32, (span, span), 1
    )
    scores = jnp.where(lower, scores, 0.0)
    for h in range(heads):
        diff = jnp.minimum(cc_ref[:, h : h + 1] - cr_ref[h : h + 1, :], 0.0)
        mix = (scores * jnp.exp(diff) * dr_ref[h : h + 1, :]).astype(BF16)
        y_ref[:, h * HEAD : (h + 1) * HEAD] = jnp.dot(
            mix, x_ref[:, h * HEAD : (h + 1) * HEAD], preferred_element_type=F32
        )


def block_spec(array):
    shape = array.shape
    return pl.BlockSpec((None,) + shape[1:], lambda i: (i,) + (0,) * (len(shape) - 1))


def per_block(kernel, shape, flops, name, *args):
    out = jax.ShapeDtypeStruct((args[0].shape[0],) + shape, F32)
    return pl.pallas_call(
        kernel,
        grid=(args[0].shape[0],),
        out_shape=out,
        in_specs=[block_spec(a) for a in args],
        out_specs=block_spec(out),
        cost_estimate=pl.CostEstimate(flops=flops, bytes_accessed=8_000_000, transcendentals=0),
        name=name,
    )(*args)


def output_kernel(
    outer, inner, grp, width, total, a_ref, w_hbm, o_ref,
    buf, w_ref, acc, sq, wsem, zsend, zrecv, xsend, xrecv, csend, crecv,
):
    z, q, x, c = places(outer, inner, grp)
    chips = grp // CORES
    g = x * CORES + c
    mate = {"grp": x * CORES + 1 - c}
    load = pltpu.make_async_copy(w_hbm, w_ref, wsem)
    load.start()

    def at_z(j):
        return {"seq": lax.rem(z + j, outer) * inner + q}

    def at_x(i):
        return {"grp": lax.rem(x + i, chips) * CORES + c}

    greet([at_z(j) for j in range(1, outer)] + [at_x(i) for i in range(1, chips)] + [mate])
    zc = {
        j: remote(
            a_ref.at[lax.rem(z + j, outer)], buf.at[g, j], zsend.at[j], zrecv.at[j], at_z(j)
        )
        for j in range(1, outer)
    }
    for j in range(1, outer):
        zc[j].start()
    xc, cc = {}, {}

    def source(j):
        return a_ref.at[z] if j == 0 else buf.at[g, j]

    def on_z(j):
        if j:
            zc[j].wait_recv()
        for i in range(1, chips):
            xc[j, i] = remote(source(j), buf.at[g, j], xsend.at[j, i - 1], xrecv.at[j, i - 1], at_x(i))
            xc[j, i].start()
        cc[j, 0] = remote(source(j), buf.at[g, j], csend.at[j, 0], crecv.at[j, 0], mate)
        cc[j, 0].start()

    def there(i, core):
        return lax.rem(x - i + chips, chips) * CORES + core

    def on_x(j):
        for i in range(1, chips):
            xc[j, i].wait_recv()
            here = buf.at[there(i, c), j]
            cc[j, i] = remote(here, here, csend.at[j, i], crecv.at[j, i], mate)
            cc[j, i].start()

    rows = acc.shape[0]
    tile = min(256, rows)

    def add(ref, gs, j, first=False):
        begin = (gs * outer + lax.rem(z - j + outer, outer)) * width
        at_w = pl.ds(pl.multiple_of(begin, 16), width)

        def some(r, carry):
            at = pl.ds(pl.multiple_of(r * tile, tile), tile)
            prod = jnp.dot(ref[at, :width], w_ref[at_w, :], preferred_element_type=F32)
            tail = ref[at, width:].astype(F32)
            square = tail[:, 0:1] + tail[:, 1:2]
            if first:
                acc[at, :] = prod
                sq[at, :] = square
            else:
                acc[at, :] += prod
                sq[at, :] += square
            return carry

        lax.fori_loop(0, rows // tile, some, 0)

    on_z(0)
    load.wait()
    add(source(0), g, 0, True)
    for j in range(1, outer + 1):
        if j < outer:
            on_z(j)
        on_x(j - 1)
        if j < outer:
            add(source(j), g, j)
        for i in range(chips):
            if i:
                add(buf.at[there(i, c), j - 1], there(i, c), j - 1)
        for i in range(chips):
            cc[j - 1, i].wait_recv()
            add(buf.at[there(i, 1 - c), j - 1], there(i, 1 - c), j - 1)
    scale = lax.rsqrt(sq[...] / total + EPS)
    o_ref[...] = (acc[...] * scale).astype(BF16)
    for j in range(outer):
        if j:
            zc[j].wait_send()
        for i in range(1, chips):
            xc[j, i].wait_send()
        for i in range(chips):
            cc[j, i].wait_send()


def emit(outer, inner, grp, width, packed, weight):
    rows, lanes = packed.shape[1:]
    chips = grp // CORES
    dma = pltpu.SemaphoreType.DMA
    hops = max(1, chips - 1)
    return pl.pallas_call(
        functools.partial(output_kernel, outer, inner, grp, width, weight.shape[0]),
        out_shape=jax.ShapeDtypeStruct((rows, weight.shape[1]), BF16),
        in_specs=[vmem(), pl.BlockSpec(memory_space=pl.ANY)],
        out_specs=vmem(),
        scratch_shapes=[
            pltpu.VMEM((grp, outer, rows, lanes), BF16),
            pltpu.VMEM(weight.shape, BF16),
            pltpu.VMEM((rows, weight.shape[1]), F32),
            pltpu.VMEM((rows, 1), F32),
            dma,
            dma((outer,)),
            dma((outer,)),
            dma((outer, hops)),
            dma((outer, hops)),
            dma((outer, chips)),
            dma((outer, chips)),
        ],
        compiler_params=pltpu.CompilerParams(
            collective_id=1, has_side_effects=True, vmem_limit_bytes=60000 * 1024
        ),
        name="emit",
    )(packed, weight)


def conv(before, current, weight):
    width = weight.shape[0]
    padded = jnp.concatenate([before, current], axis=1).astype(F32)
    length = current.shape[1]
    total = jnp.zeros(current.shape, F32)
    for offset in range(width):
        total = total + weight[offset].astype(F32) * padded[:, offset : offset + length]
    return jax.nn.silu(total).astype(BF16)


def body(
    tokens, norm_gain, inner_weight, state_weight, step_weight, step_bias, decay_rate, skip_scale,
    conv_inner, conv_state, out_gain, out_weight,
):
    seq, grp = lax.axis_size("seq"), lax.axis_size("grp")
    rows, depth = tokens.shape
    cols = inner_weight.shape[2]
    inner = next(n for n in range(1, seq + 1) if seq % n == 0 and n * cols % HEAD == 0 and n > 1)
    outer = seq // inner
    place = lax.axis_index("seq")
    z, q = place // inner, place % inner
    width = inner * cols
    heads = width // HEAD
    state = state_weight.shape[2]

    wide = tokens.astype(F32)
    normed = (
        wide * lax.rsqrt(jnp.mean(wide * wide, axis=1, keepdims=True) + EPS) * norm_gain
    ).astype(BF16)
    heads_here = step_weight.shape[1]
    small = jnp.concatenate([state_weight.reshape(depth, -1), step_weight], axis=1)
    small = jnp.pad(small, ((0, 0), (0, -small.shape[1] % 128)))
    flat = inner_weight.reshape(depth, 2 * cols)
    result, extra = project(outer, inner, grp, normed, flat, small)
    pair = result.reshape(inner, outer, rows, 2, cols)
    values_pre = jnp.moveaxis(pair[:, :, :, 0], 0, 2).reshape(outer, rows, width)
    gate = jnp.moveaxis(pair[:, :, :, 1], 0, 2).reshape(outer, rows, width)
    state_pre = extra[:, :, : 2 * state].astype(BF16)
    def mine(array):
        return lax.dynamic_slice_in_dim(array, z * (array.shape[-1] // outer), array.shape[-1] // outer, array.ndim - 1)

    raw = mine(extra[:, :, 2 * state : 2 * state + heads_here])
    delta = jax.nn.softplus(raw + mine(step_bias))
    rate, skip = mine(decay_rate), mine(skip_scale)
    logdec = -delta * rate

    taps = conv_inner.shape[0]
    last = jnp.concatenate([values_pre[:, rows - taps + 1 :], state_pre[:, rows - taps + 1 :]], axis=2)

    def around(array, steps):
        return lax.ppermute(
            array, "seq",
            [(a * inner + b, a * inner + (b + steps) % inner) for a in range(outer) for b in range(inner)],
        )

    came = around(last, 1)
    moved = jnp.concatenate([jnp.zeros_like(came[:1]), came[:-1]], axis=0)
    before = jnp.where(q == 0, moved, came)
    values = conv(before[:, :, :width], values_pre, mine(conv_inner))
    conv_out = conv(before[:, :, width:], state_pre, conv_state.reshape(taps, -1))

    blocks = rows // SPAN
    count = outer * blocks
    cumul = jnp.cumsum(logdec.reshape(count, SPAN, heads), axis=1)
    dblk = delta.reshape(count, SPAN, heads)
    ends = cumul[:, -1]
    tail = jnp.exp(ends[:, None] - cumul) * dblk
    xs = values.reshape(count, SPAN, width)
    bmat = conv_out[:, :, :state].reshape(count, SPAN, state)
    cmat = conv_out[:, :, state:].reshape(count, SPAN, state)

    update = per_block(
        functools.partial(state_kernel, heads), (width, state), 1_000_000_000, "states", xs, bmat, tail
    ).reshape(outer, blocks, width, state)
    ends = ends.reshape(outer, blocks, heads)

    def spread(array):
        return jnp.repeat(jnp.exp(array), HEAD, axis=-1)[..., None]

    final = jnp.zeros((outer, width, state), F32)
    for b in range(blocks):
        final = spread(ends[:, b]) * final + update[:, b]
    totals = jnp.sum(ends, axis=1)
    finals, sums = {0: final.astype(BF16)}, {0: totals}
    for i in range(1, inner):
        finals[i], sums[i] = around(finals[0], i), around(totals, i)

    ct = jnp.swapaxes(cumul, 1, 2)
    dt = jnp.swapaxes(dblk, 1, 2)
    intra = per_block(
        functools.partial(intra_kernel, heads), (SPAN, width), 20_000_000_000, "intra",
        xs, bmat, cmat, cumul, ct, dt,
    )

    if inner > 2:
        stack = jnp.stack([finals[i] for i in range(inner)])
        stack_sum = jnp.stack([sums[i] for i in range(inner)])
        order = (q - jnp.arange(inner)) % inner
        stack, stack_sum = stack[order], stack_sum[order]
    else:
        stack = jnp.stack([jnp.where(q == 0, finals[0], finals[1]), jnp.where(q == 0, finals[1], finals[0])])
        stack_sum = jnp.stack([jnp.where(q == 0, sums[0], sums[1]), jnp.where(q == 0, sums[1], sums[0])])
    running = jnp.zeros((width, state), F32)
    starts = []
    for a in range(outer):
        chosen = running
        for b in range(inner):
            chosen = jnp.where(q == b, running, chosen)
            running = spread(stack_sum[b, a]) * running + stack[b, a].astype(F32)
        for b in range(blocks):
            starts.append(chosen)
            if b + 1 < blocks:
                chosen = spread(ends[a, b]) * chosen + update[a, b]
    begin = jnp.stack(starts).astype(BF16)
    inter = jnp.einsum("kts,kcs->ktc", cmat, begin, preferred_element_type=F32)
    y = (
        intra
        + jnp.repeat(jnp.exp(cumul), HEAD, axis=2) * inter
        + jnp.repeat(skip, HEAD) * xs.astype(F32)
    )
    gated = y.reshape(outer, rows, width) * jax.nn.silu(gate.astype(F32))
    square = jnp.sum(gated * gated, axis=2, keepdims=True)
    high = square.astype(BF16)
    low = (square - high.astype(F32)).astype(BF16)
    lanes = -(-(width + 2) // 128) * 128
    scaled = (gated * mine(out_gain)).astype(BF16)
    packed = jnp.concatenate(
        [scaled, high, low, jnp.zeros((outer, rows, lanes - width - 2), BF16)], axis=2
    )
    return emit(outer, inner, grp, width, packed, out_weight)


def solution(mesh):
    return jax.shard_map(
        body,
        mesh=mesh,
        in_specs=(
            P("seq", None),
            P(),
            P(None, None, ("grp", "seq")),
            P(),
            P(None, "grp"),
            P("grp"),
            P("grp"),
            P("grp"),
            P(None, "grp"),
            P(),
            P("grp"),
            P(None, "grp"),
        ),
        out_specs=P("seq", "grp"),
        check_vma=False,
    )
```

```python
import functools

import jax
import jax.numpy as jnp
from jax import lax
from jax.experimental import pallas as pl
from jax.experimental.pallas import tpu as pltpu
from jax.sharding import PartitionSpec as P

SPAN = 256
HEAD = 64
HALO = 16
LANES = 128
EPS = 1e-05
CORES = 2
MESH = pl.DeviceIdType.MESH
F32 = jnp.float32
BF16 = jnp.bfloat16


def places(outer, inner, grp):
    s = lax.axis_index("seq")
    g = lax.axis_index("grp")
    return lax.div(s, inner), lax.rem(s, inner), lax.div(g, CORES), lax.rem(g, CORES)


def greet(peers):
    barrier = pltpu.get_barrier_semaphore()
    for peer in peers:
        pl.semaphore_signal(barrier, inc=1, device_id=peer, device_id_type=MESH)
    pl.semaphore_wait(barrier, len(peers))


def remote(src, dst, send, recv, peer):
    return pltpu.make_async_remote_copy(
        src_ref=src, dst_ref=dst, send_sem=send, recv_sem=recv, device_id=peer, device_id_type=MESH
    )


def project_kernel(
    outer, inner, grp, n_ref, w_ref, ws_ref, o_ref, os_ref,
    tok, wbuf, hal, wsend, wrecv, zsend, zrecv, xsend, xrecv, csend, crecv, hsend, hrecv,
):
    z, q, x, c = places(outer, inner, grp)
    chips = grp // CORES
    s, g = z * inner + q, x * CORES + c
    rows = n_ref.shape[0]
    part = rows // grp
    mate = {"grp": x * CORES + 1 - c}

    def at_z(j):
        return {"seq": lax.rem(z + j, outer) * inner + q}

    def at_q(i):
        return {"seq": z * inner + lax.rem(q + i, inner)}

    def at_x(i):
        return {"grp": lax.rem(x + i, chips) * CORES + c}

    peers = (
        [at_z(j) for j in range(1, outer)]
        + [at_q(i) for i in range(1, inner)]
        + [at_x(i) for i in range(1, chips)]
        + [mate]
    )
    greet(peers)

    def piece(index):
        return pl.ds(pl.multiple_of(index * part, part), part)

    zc = {
        j: remote(n_ref.at[piece(g)], tok.at[j - 1, piece(g)], zsend.at[j - 1], zrecv.at[j - 1], at_z(j))
        for j in range(1, outer)
    }
    wc = {
        i: remote(w_ref, wbuf.at[i - 1], wsend.at[i - 1], wrecv.at[i - 1], at_q(i))
        for i in range(1, inner)
    }
    for j in range(1, outer):
        zc[j].start()
    for i in range(1, inner):
        wc[i].start()

    hc = {}

    def lend(j):
        from_here = n_ref if j == 0 else tok.at[j - 1]
        hc[j] = remote(
            from_here.at[pl.ds(rows - HALO, HALO)], hal.at[pl.ds(j * HALO, HALO)],
            hsend.at[j], hrecv.at[j], at_q(1),
        )
        hc[j].start()

    lend(0)
    tile = min(256, rows)

    def multiply(j, pick):
        zs = lax.rem(z - j + outer, outer)

        def some(r, carry):
            at = pl.ds(pl.multiple_of(r * tile, tile), tile)
            a = n_ref[at, :] if j == 0 else tok[j - 1, at, :]
            to = pl.ds(pl.multiple_of(r * tile + HALO, HALO), tile)
            if pick == "state":
                os_ref[zs, to, :] = jnp.dot(a, ws_ref[...], preferred_element_type=F32)
            elif pick == "own":
                o_ref[q, zs, to, :] = jnp.dot(a, w_ref[...], preferred_element_type=F32).astype(BF16)
            else:
                for i in range(1, inner):
                    qs = lax.rem(q - i + inner, inner)
                    o_ref[qs, zs, to, :] = jnp.dot(
                        a, wbuf[i - 1], preferred_element_type=F32
                    ).astype(BF16)
            return carry

        lax.fori_loop(0, rows // tile, some, 0)

    xc, cc = {}, {}

    def on_z(j):
        zc[j].wait_recv()
        here = tok.at[j - 1, piece(g)]
        for i in range(1, chips):
            xc[j, i] = remote(here, here, xsend.at[j - 1, i - 1], xrecv.at[j - 1, i - 1], at_x(i))
            xc[j, i].start()
        cc[j, 0] = remote(here, here, csend.at[j - 1, 0], crecv.at[j - 1, 0], mate)
        cc[j, 0].start()

    def on_x(j):
        for i in range(1, chips):
            xc[j, i].wait_recv()
            there = lax.rem(x - i + chips, chips) * CORES + c
            here = tok.at[j - 1, piece(there)]
            cc[j, i] = remote(here, here, csend.at[j - 1, i], crecv.at[j - 1, i], mate)
            cc[j, i].start()

    multiply(0, "state")
    multiply(0, "own")
    for j in range(1, outer):
        on_z(j)
        if j > 1:
            on_x(j - 1)
    for i in range(1, inner):
        wc[i].wait_recv()
    multiply(0, "other")
    for j in range(1, outer):
        if j == outer - 1:
            on_x(j)
        for i in range(chips):
            cc[j, i].wait_recv()
        lend(j)
        multiply(j, "state")
        multiply(j, "own")
        multiply(j, "other")
    for j in range(outer):
        hc[j].wait_recv()
    wrap = jnp.where(q == 0, 1, 0)

    def place_halo(write, product):
        for j in range(outer):
            zs = lax.rem(z - j + outer, outer)
            to = lax.rem(zs + wrap, outer)
            keep = jnp.where(zs + wrap == outer, 0.0, 1.0)
            write(to, product[j * HALO : (j + 1) * HALO] * keep)

    def write_small(to, part):
        os_ref[to, :HALO, :] = part

    place_halo(write_small, jnp.dot(hal[...], ws_ref[...], preferred_element_type=F32))
    for i in range(inner):
        qs = lax.rem(q - i + inner, inner)

        def write_piece(to, part):
            o_ref[qs, to, :HALO, :] = part.astype(BF16)

        weights = w_ref[...] if i == 0 else wbuf[i - 1]
        place_halo(write_piece, jnp.dot(hal[...], weights, preferred_element_type=F32))
    for j in range(outer):
        hc[j].wait_send()
    for j in range(1, outer):
        zc[j].wait_send()
        for i in range(1, chips):
            xc[j, i].wait_send()
        for i in range(chips):
            cc[j, i].wait_send()
    for i in range(1, inner):
        wc[i].wait_send()


def vmem():
    return pl.BlockSpec(memory_space=pltpu.VMEM)


def project(outer, inner, grp, normed, weight, small):
    rows, depth = normed.shape
    chips = grp // CORES
    dma = pltpu.SemaphoreType.DMA
    hops = max(1, chips - 1)
    return pl.pallas_call(
        functools.partial(project_kernel, outer, inner, grp),
        out_shape=(
            jax.ShapeDtypeStruct((inner, outer, HALO + rows, weight.shape[1]), BF16),
            jax.ShapeDtypeStruct((outer, HALO + rows, small.shape[1]), F32),
        ),
        in_specs=[vmem()] * 3,
        out_specs=(vmem(), vmem()),
        scratch_shapes=[
            pltpu.VMEM((outer - 1, rows, depth), BF16),
            pltpu.VMEM((inner - 1,) + weight.shape, BF16),
            pltpu.VMEM((outer * HALO, depth), BF16),
            dma((inner - 1,)),
            dma((inner - 1,)),
            dma((outer - 1,)),
            dma((outer - 1,)),
            dma((outer - 1, hops)),
            dma((outer - 1, hops)),
            dma((outer - 1, chips)),
            dma((outer - 1, chips)),
            dma((outer,)),
            dma((outer,)),
        ],
        compiler_params=pltpu.CompilerParams(
            collective_id=0, has_side_effects=True, vmem_limit_bytes=60000 * 1024
        ),
        name="project",
    )(normed, weight, small)


HIGH = lax.Precision.HIGHEST


def silu(value):
    return value * jax.nn.sigmoid(value)


def taps_over(padded, weight, length):
    count = weight.shape[0]
    total = None
    for j in range(count):
        begin = HALO - count + 1 + j
        term = weight[j : j + 1, :].astype(F32) * padded[begin : begin + length, :]
        total = term if total is None else total + term
    return silu(total).astype(BF16)


def scan_kernel(
    inner, heads, state, o_ref, os_ref, ci_ref, cs_ref, bias_ref, rate_ref, skip_ref,
    y_ref, c_ref, cum_ref, u_ref, fin_ref, tot_ref, pad,
):
    rows = y_ref.shape[0]
    cols = o_ref.shape[2] // 2
    for i in range(inner):
        pad[:, i * cols : (i + 1) * cols] = o_ref[i, :, :cols].astype(F32)
    values = taps_over(pad, ci_ref, rows)
    pre = os_ref[:, : 2 * state].astype(BF16).astype(F32)
    both = taps_over(pre, cs_ref, rows)
    c_ref[...] = both[:, state:]
    delta = jax.nn.softplus(os_ref[HALO:, 2 * state :] + bias_ref[...])
    logdec = -delta * rate_ref[...]
    row = lax.broadcasted_iota(jnp.int32, (SPAN, SPAN), 0)
    lower = row >= lax.broadcasted_iota(jnp.int32, (SPAN, SPAN), 1)
    ones = jnp.where(lower, 1.0, 0.0)
    total = jnp.zeros((1, LANES), F32)
    for k in range(rows // SPAN):
        at = slice(k * SPAN, (k + 1) * SPAN)
        cum = jnp.dot(ones, logdec[at], preferred_element_type=F32, precision=HIGH)
        cum_ref[at, :] = cum
        end = cum[SPAN - 1 :, :]
        total = total + end
        here = delta[at]
        cum_rows, delta_rows = cum.T, here.T
        tail = jnp.exp(end - cum) * here
        b, c = both[at, :state], both[at, state:]
        scores = lax.dot_general(c, b, (((1,), (1,)), ((), ())), preferred_element_type=F32)
        scores = jnp.where(lower, scores, 0.0)
        wide_b = b.astype(F32)
        for h in range(heads):
            span = slice(h * HEAD, (h + 1) * HEAD)
            x = values[at, span]
            diff = jnp.minimum(cum[:, h : h + 1] - cum_rows[h : h + 1, :], 0.0)
            mix = (scores * jnp.exp(diff) * delta_rows[h : h + 1, :]).astype(BF16)
            y_ref[at, span] = jnp.dot(mix, x, preferred_element_type=F32) + skip_ref[
                :, h : h + 1
            ] * x.astype(F32)
            weighted = (tail[:, h : h + 1] * wide_b).astype(BF16)
            update = lax.dot_general(
                x, weighted, (((0,), (0,)), ((), ())), preferred_element_type=F32
            )
            u_ref[k, span, :] = update
            if k:
                update = update + jnp.exp(end[:, h : h + 1]) * held[h]
            else:
                held = {} if h == 0 else held
            held[h] = update
    for h in range(heads):
        fin_ref[h * HEAD : (h + 1) * HEAD, :] = held[h].astype(BF16)
    tot_ref[...] = jnp.broadcast_to(total, tot_ref.shape)


def join_kernel(
    inner, heads, state, y_ref, c_ref, cum_ref, u_ref, fin_ref, tot_ref, o_ref, gain_ref,
    p_ref, running, chosen, gate, merged,
):
    rows = y_ref.shape[0]
    cols = o_ref.shape[2] // 2
    width = heads * HEAD
    q = lax.rem(lax.axis_index("seq"), inner)

    @pl.when(pl.program_id(0) == 0)
    def _():
        running[...] = jnp.zeros_like(running)

    def decay(row, source):
        for h in range(heads):
            span = slice(h * HEAD, (h + 1) * HEAD)
            yield span, jnp.exp(row[:, h : h + 1]) * source[span, :]

    for b in range(inner):
        @pl.when(q == b)
        def _():
            chosen[...] = running[...]

        rel = lax.rem(q - b + inner, inner)
        row = tot_ref[rel, 0:1, :]
        for span, old in decay(row, running):
            running[span, :] = old + fin_ref[rel, span, :].astype(F32)
    for i in range(inner):
        gate[:, i * cols : (i + 1) * cols] = o_ref[i, HALO:, cols:].astype(F32)
    blocks = rows // SPAN
    for k in range(blocks):
        at = slice(k * SPAN, (k + 1) * SPAN)
        inter = lax.dot_general(
            c_ref[at, :], chosen[...].astype(BF16), (((1,), (1,)), ((), ())),
            preferred_element_type=F32,
        )
        cum = cum_ref[at, :]
        grow = jnp.exp(cum)
        for h in range(heads):
            span = slice(h * HEAD, (h + 1) * HEAD)
            merged[at, span] = y_ref[at, span] + grow[:, h : h + 1] * inter[:, span]
        if k + 1 < blocks:
            for span, old in decay(cum[SPAN - 1 :, :], chosen):
                chosen[span, :] = old + u_ref[k, span, :]
    gated = merged[...] * silu(gate[...])
    square = jnp.sum(gated * gated, axis=1, keepdims=True)
    high = square.astype(BF16).astype(F32)
    low = square - high
    p_ref[:, :width] = (gated * gain_ref[...]).astype(BF16)
    extra = p_ref.shape[1] - width
    lane = lax.broadcasted_iota(jnp.int32, (rows, extra), 1)
    p_ref[:, width:] = jnp.where(lane == 0, high, jnp.where(lane == 1, low, 0.0)).astype(BF16)


def stepped(array, axis):
    shape = array.shape
    block = shape[:axis] + (None,) + shape[axis + 1 :]

    def index(i):
        return (0,) * axis + (i,) + (0,) * (len(shape) - axis - 1)

    return pl.BlockSpec(block, index)


def whole(array):
    return pl.BlockSpec(array.shape, lambda i: (0,) * len(array.shape))


def per_shard(kernel, outer, outs, moving, fixed, scratch, name):
    specs = [stepped(a, axis) for a, axis in moving] + [whole(a) for a in fixed]
    return pl.pallas_call(
        kernel,
        grid=(outer,),
        out_shape=outs,
        in_specs=specs,
        out_specs=[stepped(a, 0) for a in outs],
        scratch_shapes=scratch,
        compiler_params=pltpu.CompilerParams(vmem_limit_bytes=50000 * 1024),
        cost_estimate=pl.CostEstimate(
            flops=10_000_000_000, bytes_accessed=8_000_000, transcendentals=0
        ),
        name=name,
    )(*[a for a, _ in moving], *fixed)


def output_kernel(
    outer, inner, grp, width, total, a_ref, w_hbm, o_ref,
    buf, w_ref, acc, sq, wsem, zsend, zrecv, xsend, xrecv, csend, crecv,
):
    z, q, x, c = places(outer, inner, grp)
    chips = grp // CORES
    g = x * CORES + c
    mate = {"grp": x * CORES + 1 - c}
    load = pltpu.make_async_copy(w_hbm, w_ref, wsem)
    load.start()

    def at_z(j):
        return {"seq": lax.rem(z + j, outer) * inner + q}

    def at_x(i):
        return {"grp": lax.rem(x + i, chips) * CORES + c}

    greet([at_z(j) for j in range(1, outer)] + [at_x(i) for i in range(1, chips)] + [mate])
    zc = {
        j: remote(
            a_ref.at[lax.rem(z + j, outer)], buf.at[g, j], zsend.at[j], zrecv.at[j], at_z(j)
        )
        for j in range(1, outer)
    }
    for j in range(1, outer):
        zc[j].start()
    xc, cc = {}, {}

    def source(j):
        return a_ref.at[z] if j == 0 else buf.at[g, j]

    def on_z(j):
        if j:
            zc[j].wait_recv()
        for i in range(1, chips):
            xc[j, i] = remote(source(j), buf.at[g, j], xsend.at[j, i - 1], xrecv.at[j, i - 1], at_x(i))
            xc[j, i].start()
        cc[j, 0] = remote(source(j), buf.at[g, j], csend.at[j, 0], crecv.at[j, 0], mate)
        cc[j, 0].start()

    def there(i, core):
        return lax.rem(x - i + chips, chips) * CORES + core

    def on_x(j):
        for i in range(1, chips):
            xc[j, i].wait_recv()
            here = buf.at[there(i, c), j]
            cc[j, i] = remote(here, here, csend.at[j, i], crecv.at[j, i], mate)
            cc[j, i].start()

    rows = acc.shape[0]
    tile = min(256, rows)

    def add(ref, gs, j, first=False):
        begin = (gs * outer + lax.rem(z - j + outer, outer)) * width
        at_w = pl.ds(pl.multiple_of(begin, 16), width)

        def some(r, carry):
            at = pl.ds(pl.multiple_of(r * tile, tile), tile)
            prod = jnp.dot(ref[at, :width], w_ref[at_w, :], preferred_element_type=F32)
            tail = ref[at, width:].astype(F32)
            square = tail[:, 0:1] + tail[:, 1:2]
            if first:
                acc[at, :] = prod
                sq[at, :] = square
            else:
                acc[at, :] += prod
                sq[at, :] += square
            return carry

        lax.fori_loop(0, rows // tile, some, 0)

    on_z(0)
    load.wait()
    add(source(0), g, 0, True)
    for j in range(1, outer + 1):
        if j < outer:
            on_z(j)
        on_x(j - 1)
        if j < outer:
            add(source(j), g, j)
        for i in range(chips):
            if i:
                add(buf.at[there(i, c), j - 1], there(i, c), j - 1)
        for i in range(chips):
            cc[j - 1, i].wait_recv()
            add(buf.at[there(i, 1 - c), j - 1], there(i, 1 - c), j - 1)
    scale = lax.rsqrt(sq[...] / total + EPS)
    o_ref[...] = (acc[...] * scale).astype(BF16)
    for j in range(outer):
        if j:
            zc[j].wait_send()
        for i in range(1, chips):
            xc[j, i].wait_send()
        for i in range(chips):
            cc[j, i].wait_send()


def emit(outer, inner, grp, width, packed, weight):
    rows, lanes = packed.shape[1:]
    chips = grp // CORES
    dma = pltpu.SemaphoreType.DMA
    hops = max(1, chips - 1)
    return pl.pallas_call(
        functools.partial(output_kernel, outer, inner, grp, width, weight.shape[0]),
        out_shape=jax.ShapeDtypeStruct((rows, weight.shape[1]), BF16),
        in_specs=[vmem(), pl.BlockSpec(memory_space=pl.ANY)],
        out_specs=vmem(),
        scratch_shapes=[
            pltpu.VMEM((grp, outer, rows, lanes), BF16),
            pltpu.VMEM(weight.shape, BF16),
            pltpu.VMEM((rows, weight.shape[1]), F32),
            pltpu.VMEM((rows, 1), F32),
            dma,
            dma((outer,)),
            dma((outer,)),
            dma((outer, hops)),
            dma((outer, hops)),
            dma((outer, chips)),
            dma((outer, chips)),
        ],
        compiler_params=pltpu.CompilerParams(
            collective_id=1, has_side_effects=True, vmem_limit_bytes=60000 * 1024
        ),
        name="emit",
    )(packed, weight)


def body(
    tokens, norm_gain, inner_weight, state_weight, step_weight, step_bias, decay_rate, skip_scale,
    conv_inner, conv_state, out_gain, out_weight,
):
    seq, grp = lax.axis_size("seq"), lax.axis_size("grp")
    rows, depth = tokens.shape
    cols = inner_weight.shape[2]
    inner = next(n for n in range(1, seq + 1) if seq % n == 0 and n * cols % HEAD == 0 and n > 1)
    outer = seq // inner
    place = lax.axis_index("seq")
    z, q = place // inner, place % inner
    width = inner * cols
    heads = width // HEAD
    state = state_weight.shape[2]

    wide = tokens.astype(F32)
    normed = (
        wide * lax.rsqrt(jnp.mean(wide * wide, axis=1, keepdims=True) + EPS) * norm_gain
    ).astype(BF16)

    def mine(array):
        size = array.shape[-1] // outer
        return lax.dynamic_slice_in_dim(array, z * size, size, array.ndim - 1)

    def lane_row(array):
        return jnp.pad(mine(array), (0, LANES - heads))[None]

    small = jnp.concatenate([state_weight.reshape(depth, -1), mine(step_weight)], axis=1)
    small = jnp.pad(small, ((0, 0), (0, -small.shape[1] % LANES)))
    flat = inner_weight.reshape(depth, 2 * cols)
    result, extra = project(outer, inner, grp, normed, flat, small)

    def around(array, steps):
        return lax.ppermute(
            array, "seq",
            [(a * inner + b, a * inner + (b + steps) % inner) for a in range(outer) for b in range(inner)],
        )

    blocks = rows // SPAN
    shape = jax.ShapeDtypeStruct
    y, cmat, cumul, update, final, totals = per_shard(
        functools.partial(scan_kernel, inner, heads, state),
        outer,
        [
            shape((outer, rows, width), F32),
            shape((outer, rows, state), BF16),
            shape((outer, rows, LANES), F32),
            shape((outer, blocks, width, state), F32),
            shape((outer, width, state), BF16),
            shape((outer, 8, LANES), F32),
        ],
        [(result, 1), (extra, 0)],
        [
            mine(conv_inner),
            conv_state.reshape(conv_state.shape[0], -1),
            lane_row(step_bias),
            lane_row(decay_rate),
            lane_row(skip_scale),
        ],
        [pltpu.VMEM((HALO + rows, width), F32)],
        "scan",
    )
    finals = jnp.stack([final] + [around(final, i) for i in range(1, inner)])
    sums = jnp.stack([totals] + [around(totals, i) for i in range(1, inner)])
    lanes = -(-(width + 2) // LANES) * LANES
    (packed,) = per_shard(
        functools.partial(join_kernel, inner, heads, state),
        outer,
        [shape((outer, rows, lanes), BF16)],
        [(y, 0), (cmat, 0), (cumul, 0), (update, 0), (finals, 1), (sums, 1), (result, 1)],
        [mine(out_gain)[None]],
        [
            pltpu.VMEM((width, state), F32),
            pltpu.VMEM((width, state), F32),
            pltpu.VMEM((rows, width), F32),
            pltpu.VMEM((rows, width), F32),
        ],
        "join",
    )
    return emit(outer, inner, grp, width, packed, out_weight)


def solution(mesh):
    return jax.shard_map(
        body,
        mesh=mesh,
        in_specs=(
            P("seq", None),
            P(),
            P(None, None, ("grp", "seq")),
            P(),
            P(None, "grp"),
            P("grp"),
            P("grp"),
            P("grp"),
            P(None, "grp"),
            P(),
            P("grp"),
            P(None, "grp"),
        ),
        out_specs=P("seq", "grp"),
        check_vma=False,
    )
```

```python
import functools

import jax
import jax.numpy as jnp
from jax import lax
from jax.experimental import pallas as pl
from jax.experimental.pallas import tpu as pltpu
from jax.sharding import PartitionSpec as P

SPAN = 256
HEAD = 64
HALO = 16
LANES = 128
EPS = 1e-05
CORES = 2
MESH = pl.DeviceIdType.MESH
F32 = jnp.float32
BF16 = jnp.bfloat16


def places(outer, inner, grp):
    s = lax.axis_index("seq")
    g = lax.axis_index("grp")
    return lax.div(s, inner), lax.rem(s, inner), lax.div(g, CORES), lax.rem(g, CORES)


def flip(z, j):
    for bit in range(j.bit_length()):
        if (j >> bit) % 2:
            z = z + 2**bit - 2 ** (bit + 1) * lax.rem(lax.div(z, 2**bit), 2)
    return z


def greet(peers):
    barrier = pltpu.get_barrier_semaphore()
    for peer in peers:
        pl.semaphore_signal(barrier, inc=1, device_id=peer, device_id_type=MESH)
    pl.semaphore_wait(barrier, len(peers))


def remote(src, dst, send, recv, peer):
    return pltpu.make_async_remote_copy(
        src_ref=src, dst_ref=dst, send_sem=send, recv_sem=recv, device_id=peer, device_id_type=MESH
    )


def project_kernel(
    outer, inner, grp, n_ref, w_ref, ws_ref, o_ref, os_ref,
    tok, wbuf, hal, wsend, wrecv, zsend, zrecv, xsend, xrecv, csend, crecv, hsend, hrecv,
):
    z, q, x, c = places(outer, inner, grp)
    chips = grp // CORES
    s, g = z * inner + q, x * CORES + c
    rows = n_ref.shape[0]
    part = rows // grp
    mate = {"grp": x * CORES + 1 - c}

    def at_z(j):
        return {"seq": flip(z, j) * inner + q}

    def at_q(i):
        return {"seq": z * inner + lax.rem(q + i, inner)}

    def at_x(i):
        return {"grp": lax.rem(x + i, chips) * CORES + c}

    peers = (
        [at_z(j) for j in range(1, outer)]
        + [at_q(i) for i in range(1, inner)]
        + [at_x(i) for i in range(1, chips)]
        + [mate]
    )
    greet(peers)

    def piece(index):
        return pl.ds(pl.multiple_of(index * part, part), part)

    zc = {
        j: remote(n_ref.at[piece(g)], tok.at[j - 1, piece(g)], zsend.at[j - 1], zrecv.at[j - 1], at_z(j))
        for j in range(1, outer)
    }
    wc = {
        i: remote(w_ref, wbuf.at[i - 1], wsend.at[i - 1], wrecv.at[i - 1], at_q(i))
        for i in range(1, inner)
    }
    for j in range(1, outer):
        zc[j].start()
    for i in range(1, inner):
        wc[i].start()

    hc = {}

    def lend(j):
        from_here = n_ref if j == 0 else tok.at[j - 1]
        hc[j] = remote(
            from_here.at[pl.ds(rows - HALO, HALO)], hal.at[pl.ds(j * HALO, HALO)],
            hsend.at[j], hrecv.at[j], at_q(1),
        )
        hc[j].start()

    lend(0)
    tile = min(256, rows)

    def multiply(j, pick):
        zs = flip(z, j)

        def some(r, carry):
            at = pl.ds(pl.multiple_of(r * tile, tile), tile)
            a = n_ref[at, :] if j == 0 else tok[j - 1, at, :]
            to = pl.ds(pl.multiple_of(r * tile + HALO, HALO), tile)
            if pick == "state":
                os_ref[zs, to, :] = jnp.dot(a, ws_ref[...], preferred_element_type=F32)
            elif pick == "own":
                o_ref[q, zs, to, :] = jnp.dot(a, w_ref[...], preferred_element_type=F32).astype(BF16)
            else:
                for i in range(1, inner):
                    qs = lax.rem(q - i + inner, inner)
                    o_ref[qs, zs, to, :] = jnp.dot(
                        a, wbuf[i - 1], preferred_element_type=F32
                    ).astype(BF16)
            return carry

        lax.fori_loop(0, rows // tile, some, 0)

    xc, cc = {}, {}

    def on_z(j):
        zc[j].wait_recv()
        here = tok.at[j - 1, piece(g)]
        for i in range(1, chips):
            xc[j, i] = remote(here, here, xsend.at[j - 1, i - 1], xrecv.at[j - 1, i - 1], at_x(i))
            xc[j, i].start()
        cc[j, 0] = remote(here, here, csend.at[j - 1, 0], crecv.at[j - 1, 0], mate)
        cc[j, 0].start()

    def on_x(j):
        for i in range(1, chips):
            xc[j, i].wait_recv()
            there = lax.rem(x - i + chips, chips) * CORES + c
            here = tok.at[j - 1, piece(there)]
            cc[j, i] = remote(here, here, csend.at[j - 1, i], crecv.at[j - 1, i], mate)
            cc[j, i].start()

    multiply(0, "state")
    multiply(0, "own")
    for j in range(1, outer):
        on_z(j)
        if j > 1:
            on_x(j - 1)
    for i in range(1, inner):
        wc[i].wait_recv()
    multiply(0, "other")
    for j in range(1, outer):
        if j == outer - 1:
            on_x(j)
        for i in range(chips):
            cc[j, i].wait_recv()
        lend(j)
        multiply(j, "state")
        multiply(j, "own")
        multiply(j, "other")
    for j in range(outer):
        hc[j].wait_recv()
    wrap = jnp.where(q == 0, 1, 0)

    def place_halo(write, product):
        for j in range(outer):
            zs = flip(z, j)
            to = lax.rem(zs + wrap, outer)
            keep = jnp.where(zs + wrap == outer, 0.0, 1.0)
            write(to, product[j * HALO : (j + 1) * HALO] * keep)

    def write_small(to, part):
        os_ref[to, :HALO, :] = part

    place_halo(write_small, jnp.dot(hal[...], ws_ref[...], preferred_element_type=F32))
    for i in range(inner):
        qs = lax.rem(q - i + inner, inner)

        def write_piece(to, part):
            o_ref[qs, to, :HALO, :] = part.astype(BF16)

        weights = w_ref[...] if i == 0 else wbuf[i - 1]
        place_halo(write_piece, jnp.dot(hal[...], weights, preferred_element_type=F32))
    for j in range(outer):
        hc[j].wait_send()
    for j in range(1, outer):
        zc[j].wait_send()
        for i in range(1, chips):
            xc[j, i].wait_send()
        for i in range(chips):
            cc[j, i].wait_send()
    for i in range(1, inner):
        wc[i].wait_send()


def vmem():
    return pl.BlockSpec(memory_space=pltpu.VMEM)


def project(outer, inner, grp, normed, weight, small):
    rows, depth = normed.shape
    chips = grp // CORES
    dma = pltpu.SemaphoreType.DMA
    hops = max(1, chips - 1)
    return pl.pallas_call(
        functools.partial(project_kernel, outer, inner, grp),
        out_shape=(
            jax.ShapeDtypeStruct((inner, outer, HALO + rows, weight.shape[1]), BF16),
            jax.ShapeDtypeStruct((outer, HALO + rows, small.shape[1]), F32),
        ),
        in_specs=[vmem()] * 3,
        out_specs=(vmem(), vmem()),
        scratch_shapes=[
            pltpu.VMEM((outer - 1, rows, depth), BF16),
            pltpu.VMEM((inner - 1,) + weight.shape, BF16),
            pltpu.VMEM((outer * HALO, depth), BF16),
            dma((inner - 1,)),
            dma((inner - 1,)),
            dma((outer - 1,)),
            dma((outer - 1,)),
            dma((outer - 1, hops)),
            dma((outer - 1, hops)),
            dma((outer - 1, chips)),
            dma((outer - 1, chips)),
            dma((outer,)),
            dma((outer,)),
        ],
        compiler_params=pltpu.CompilerParams(
            collective_id=0, has_side_effects=True, vmem_limit_bytes=60000 * 1024
        ),
        name="project",
    )(normed, weight, small)


HIGH = lax.Precision.HIGHEST


def silu(value):
    return value * jax.nn.sigmoid(value)


def taps_over(padded, weight, length):
    count = weight.shape[0]
    total = None
    for j in range(count):
        begin = HALO - count + 1 + j
        term = weight[j : j + 1, :].astype(F32) * padded[begin : begin + length, :]
        total = term if total is None else total + term
    return silu(total).astype(BF16)


def scan_kernel(
    inner, heads, state, o_ref, os_ref, ci_ref, cs_ref, bias_ref, rate_ref, skip_ref,
    y_ref, c_ref, cum_ref, u_ref, fin_ref, tot_ref, pad,
):
    rows = y_ref.shape[0]
    cols = o_ref.shape[2] // 2
    for i in range(inner):
        pad[:, i * cols : (i + 1) * cols] = o_ref[i, :, :cols].astype(F32)
    values = taps_over(pad, ci_ref, rows)
    pre = os_ref[:, : 2 * state].astype(BF16).astype(F32)
    both = taps_over(pre, cs_ref, rows)
    c_ref[...] = both[:, state:]
    delta = jax.nn.softplus(os_ref[HALO:, 2 * state :] + bias_ref[...])
    logdec = -delta * rate_ref[...]
    row = lax.broadcasted_iota(jnp.int32, (SPAN, SPAN), 0)
    lower = row >= lax.broadcasted_iota(jnp.int32, (SPAN, SPAN), 1)
    ones = jnp.where(lower, 1.0, 0.0)
    total = jnp.zeros((1, LANES), F32)
    for k in range(rows // SPAN):
        at = slice(k * SPAN, (k + 1) * SPAN)
        cum = jnp.dot(ones, logdec[at], preferred_element_type=F32, precision=HIGH)
        cum_ref[at, :] = cum
        end = cum[SPAN - 1 :, :]
        total = total + end
        here = delta[at]
        cum_rows, delta_rows = cum.T, here.T
        tail = jnp.exp(end - cum) * here
        b, c = both[at, :state], both[at, state:]
        scores = lax.dot_general(c, b, (((1,), (1,)), ((), ())), preferred_element_type=F32)
        scores = jnp.where(lower, scores, 0.0)
        wide_b = b.astype(F32)
        for h in range(heads):
            span = slice(h * HEAD, (h + 1) * HEAD)
            x = values[at, span]
            diff = jnp.minimum(cum[:, h : h + 1] - cum_rows[h : h + 1, :], 0.0)
            mix = (scores * jnp.exp(diff) * delta_rows[h : h + 1, :]).astype(BF16)
            y_ref[at, span] = jnp.dot(mix, x, preferred_element_type=F32) + skip_ref[
                :, h : h + 1
            ] * x.astype(F32)
            weighted = (tail[:, h : h + 1] * wide_b).astype(BF16)
            update = lax.dot_general(
                x, weighted, (((0,), (0,)), ((), ())), preferred_element_type=F32
            )
            u_ref[k, span, :] = update
            if k:
                update = update + jnp.exp(end[:, h : h + 1]) * held[h]
            else:
                held = {} if h == 0 else held
            held[h] = update
    for h in range(heads):
        fin_ref[h * HEAD : (h + 1) * HEAD, :] = held[h].astype(BF16)
    tot_ref[...] = jnp.broadcast_to(total, tot_ref.shape)


def join_kernel(
    inner, heads, state, y_ref, c_ref, cum_ref, u_ref, fin_ref, tot_ref, o_ref, gain_ref,
    p_ref, running, chosen, gate, merged,
):
    rows = y_ref.shape[0]
    cols = o_ref.shape[2] // 2
    width = heads * HEAD
    q = lax.rem(lax.axis_index("seq"), inner)

    @pl.when(pl.program_id(0) == 0)
    def _():
        running[...] = jnp.zeros_like(running)

    def decay(row, source):
        for h in range(heads):
            span = slice(h * HEAD, (h + 1) * HEAD)
            yield span, jnp.exp(row[:, h : h + 1]) * source[span, :]

    for b in range(inner):
        @pl.when(q == b)
        def _():
            chosen[...] = running[...]

        rel = lax.rem(q - b + inner, inner)
        row = tot_ref[rel, 0:1, :]
        for span, old in decay(row, running):
            running[span, :] = old + fin_ref[rel, span, :].astype(F32)
    for i in range(inner):
        gate[:, i * cols : (i + 1) * cols] = o_ref[i, HALO:, cols:].astype(F32)
    blocks = rows // SPAN
    for k in range(blocks):
        at = slice(k * SPAN, (k + 1) * SPAN)
        inter = lax.dot_general(
            c_ref[at, :], chosen[...].astype(BF16), (((1,), (1,)), ((), ())),
            preferred_element_type=F32,
        )
        cum = cum_ref[at, :]
        grow = jnp.exp(cum)
        for h in range(heads):
            span = slice(h * HEAD, (h + 1) * HEAD)
            merged[at, span] = y_ref[at, span] + grow[:, h : h + 1] * inter[:, span]
        if k + 1 < blocks:
            for span, old in decay(cum[SPAN - 1 :, :], chosen):
                chosen[span, :] = old + u_ref[k, span, :]
    gated = merged[...] * silu(gate[...])
    square = jnp.sum(gated * gated, axis=1, keepdims=True)
    high = square.astype(BF16).astype(F32)
    low = square - high
    p_ref[:, :width] = (gated * gain_ref[...]).astype(BF16)
    extra = p_ref.shape[1] - width
    lane = lax.broadcasted_iota(jnp.int32, (rows, extra), 1)
    p_ref[:, width:] = jnp.where(lane == 0, high, jnp.where(lane == 1, low, 0.0)).astype(BF16)


def stepped(array, axis):
    shape = array.shape
    block = shape[:axis] + (None,) + shape[axis + 1 :]

    def index(i):
        return (0,) * axis + (i,) + (0,) * (len(shape) - axis - 1)

    return pl.BlockSpec(block, index)


def whole(array):
    return pl.BlockSpec(array.shape, lambda i: (0,) * len(array.shape))


def per_shard(kernel, outer, outs, moving, fixed, scratch, name):
    specs = [stepped(a, axis) for a, axis in moving] + [whole(a) for a in fixed]
    return pl.pallas_call(
        kernel,
        grid=(outer,),
        out_shape=outs,
        in_specs=specs,
        out_specs=[stepped(a, 0) for a in outs],
        scratch_shapes=scratch,
        compiler_params=pltpu.CompilerParams(vmem_limit_bytes=50000 * 1024),
        cost_estimate=pl.CostEstimate(
            flops=10_000_000_000, bytes_accessed=8_000_000, transcendentals=0
        ),
        name=name,
    )(*[a for a, _ in moving], *fixed)


def output_kernel(
    outer, inner, grp, width, total, a_ref, w_hbm, o_ref,
    buf, w_ref, acc, sq, wsem, zsend, zrecv, xsend, xrecv, csend, crecv,
):
    z, q, x, c = places(outer, inner, grp)
    chips = grp // CORES
    g = x * CORES + c
    mate = {"grp": x * CORES + 1 - c}
    load = pltpu.make_async_copy(w_hbm, w_ref, wsem)
    load.start()

    def at_z(j):
        return {"seq": flip(z, j) * inner + q}

    def at_x(i):
        return {"grp": lax.rem(x + i, chips) * CORES + c}

    greet([at_z(j) for j in range(1, outer)] + [at_x(i) for i in range(1, chips)] + [mate])
    zc = {
        j: remote(
            a_ref.at[flip(z, j)], buf.at[g, j], zsend.at[j], zrecv.at[j], at_z(j)
        )
        for j in range(1, outer)
    }
    for j in range(1, outer):
        zc[j].start()
    xc, cc = {}, {}

    def source(j):
        return a_ref.at[z] if j == 0 else buf.at[g, j]

    def on_z(j):
        if j:
            zc[j].wait_recv()
        for i in range(1, chips):
            xc[j, i] = remote(source(j), buf.at[g, j], xsend.at[j, i - 1], xrecv.at[j, i - 1], at_x(i))
            xc[j, i].start()
        cc[j, 0] = remote(source(j), buf.at[g, j], csend.at[j, 0], crecv.at[j, 0], mate)
        cc[j, 0].start()

    def there(i, core):
        return lax.rem(x - i + chips, chips) * CORES + core

    def on_x(j):
        for i in range(1, chips):
            xc[j, i].wait_recv()
            here = buf.at[there(i, c), j]
            cc[j, i] = remote(here, here, csend.at[j, i], crecv.at[j, i], mate)
            cc[j, i].start()

    rows = acc.shape[0]
    tile = min(256, rows)

    def add(ref, gs, j, first=False):
        begin = (gs * outer + flip(z, j)) * width
        at_w = pl.ds(pl.multiple_of(begin, 16), width)

        def some(r, carry):
            at = pl.ds(pl.multiple_of(r * tile, tile), tile)
            prod = jnp.dot(ref[at, :width], w_ref[at_w, :], preferred_element_type=F32)
            tail = ref[at, width:].astype(F32)
            square = tail[:, 0:1] + tail[:, 1:2]
            if first:
                acc[at, :] = prod
                sq[at, :] = square
            else:
                acc[at, :] += prod
                sq[at, :] += square
            return carry

        lax.fori_loop(0, rows // tile, some, 0)

    on_z(0)
    load.wait()
    add(source(0), g, 0, True)
    for j in range(1, outer + 1):
        if j < outer:
            on_z(j)
        on_x(j - 1)
        if j < outer:
            add(source(j), g, j)
        for i in range(chips):
            if i:
                add(buf.at[there(i, c), j - 1], there(i, c), j - 1)
        for i in range(chips):
            cc[j - 1, i].wait_recv()
            add(buf.at[there(i, 1 - c), j - 1], there(i, 1 - c), j - 1)
    scale = lax.rsqrt(sq[...] / total + EPS)
    o_ref[...] = (acc[...] * scale).astype(BF16)
    for j in range(outer):
        if j:
            zc[j].wait_send()
        for i in range(1, chips):
            xc[j, i].wait_send()
        for i in range(chips):
            cc[j, i].wait_send()


def emit(outer, inner, grp, width, packed, weight):
    rows, lanes = packed.shape[1:]
    chips = grp // CORES
    dma = pltpu.SemaphoreType.DMA
    hops = max(1, chips - 1)
    return pl.pallas_call(
        functools.partial(output_kernel, outer, inner, grp, width, weight.shape[0]),
        out_shape=jax.ShapeDtypeStruct((rows, weight.shape[1]), BF16),
        in_specs=[vmem(), pl.BlockSpec(memory_space=pl.ANY)],
        out_specs=vmem(),
        scratch_shapes=[
            pltpu.VMEM((grp, outer, rows, lanes), BF16),
            pltpu.VMEM(weight.shape, BF16),
            pltpu.VMEM((rows, weight.shape[1]), F32),
            pltpu.VMEM((rows, 1), F32),
            dma,
            dma((outer,)),
            dma((outer,)),
            dma((outer, hops)),
            dma((outer, hops)),
            dma((outer, chips)),
            dma((outer, chips)),
        ],
        compiler_params=pltpu.CompilerParams(
            collective_id=1, has_side_effects=True, vmem_limit_bytes=60000 * 1024
        ),
        name="emit",
    )(packed, weight)


def body(
    tokens, norm_gain, inner_weight, state_weight, step_weight, step_bias, decay_rate, skip_scale,
    conv_inner, conv_state, out_gain, out_weight,
):
    seq, grp = lax.axis_size("seq"), lax.axis_size("grp")
    rows, depth = tokens.shape
    cols = inner_weight.shape[2]
    inner = next(n for n in range(1, seq + 1) if seq % n == 0 and n * cols % HEAD == 0 and n > 1)
    outer = seq // inner
    assert outer & (outer - 1) == 0
    place = lax.axis_index("seq")
    z, q = place // inner, place % inner
    width = inner * cols
    heads = width // HEAD
    state = state_weight.shape[2]

    wide = tokens.astype(F32)
    normed = (
        wide * lax.rsqrt(jnp.mean(wide * wide, axis=1, keepdims=True) + EPS) * norm_gain
    ).astype(BF16)

    def mine(array):
        size = array.shape[-1] // outer
        return lax.dynamic_slice_in_dim(array, z * size, size, array.ndim - 1)

    def lane_row(array):
        return jnp.pad(mine(array), (0, LANES - heads))[None]

    small = jnp.concatenate([state_weight.reshape(depth, -1), mine(step_weight)], axis=1)
    small = jnp.pad(small, ((0, 0), (0, -small.shape[1] % LANES)))
    flat = inner_weight.reshape(depth, 2 * cols)
    result, extra = project(outer, inner, grp, normed, flat, small)

    def around(array, steps):
        return lax.ppermute(
            array, "seq",
            [(a * inner + b, a * inner + (b + steps) % inner) for a in range(outer) for b in range(inner)],
        )

    blocks = rows // SPAN
    shape = jax.ShapeDtypeStruct
    y, cmat, cumul, update, final, totals = per_shard(
        functools.partial(scan_kernel, inner, heads, state),
        outer,
        [
            shape((outer, rows, width), F32),
            shape((outer, rows, state), BF16),
            shape((outer, rows, LANES), F32),
            shape((outer, blocks, width, state), F32),
            shape((outer, width, state), BF16),
            shape((outer, 8, LANES), F32),
        ],
        [(result, 1), (extra, 0)],
        [
            mine(conv_inner),
            conv_state.reshape(conv_state.shape[0], -1),
            lane_row(step_bias),
            lane_row(decay_rate),
            lane_row(skip_scale),
        ],
        [pltpu.VMEM((HALO + rows, width), F32)],
        "scan",
    )
    finals = jnp.stack([final] + [around(final, i) for i in range(1, inner)])
    sums = jnp.stack([totals] + [around(totals, i) for i in range(1, inner)])
    lanes = -(-(width + 2) // LANES) * LANES
    (packed,) = per_shard(
        functools.partial(join_kernel, inner, heads, state),
        outer,
        [shape((outer, rows, lanes), BF16)],
        [(y, 0), (cmat, 0), (cumul, 0), (update, 0), (finals, 1), (sums, 1), (result, 1)],
        [mine(out_gain)[None]],
        [
            pltpu.VMEM((width, state), F32),
            pltpu.VMEM((width, state), F32),
            pltpu.VMEM((rows, width), F32),
            pltpu.VMEM((rows, width), F32),
        ],
        "join",
    )
    return emit(outer, inner, grp, width, packed, out_weight)


def solution(mesh):
    return jax.shard_map(
        body,
        mesh=mesh,
        in_specs=(
            P("seq", None),
            P(),
            P(None, None, ("grp", "seq")),
            P(),
            P(None, "grp"),
            P("grp"),
            P("grp"),
            P("grp"),
            P(None, "grp"),
            P(),
            P("grp"),
            P(None, "grp"),
        ),
        out_specs=P("seq", "grp"),
        check_vma=False,
    )
```
